32 devices in a mesh: grp: 2 (over x), det: 8 (over z, y), wlk: 2 (over core).
Axes of the slice: x: 2, y: 2, z: 4, core: 2. Of those that a mesh axis runs over, the one named last changes fastest.
Arguments:
- greens: bfloat16 [32, 450, 150], P(('grp', 'det', 'wlk')), parts along dimension 0, may hold values from -2 to 2
- chol_vectors: bfloat16 [1024, 450, 150], P(('grp', 'det')), parts along dimension 0, may hold values from -0.0234375 to 0.0234375
- hole_orbitals: int32 [2048, 4], P(('grp', 'det')), parts along dimension 0, may hold values from 0 to 63, as said below
- particle_orbitals: int32 [2048, 4], P(('grp', 'det')), parts along dimension 0, may hold values from 0 to 63, as said below
- excitation_order: int32 [2048], P(('grp', 'det')), parts along dimension 0, may hold values from 0 to 4
- amplitudes: float32 [2048], P(('grp', 'det')), parts along dimension 0, may hold values from -0.6 to 0.6
Outputs:
- correlation: float32 [32], P(('grp', 'det', 'wlk')), parts along dimension 0
- force_bias: float32 [32, 512], P(('grp', 'det', 'wlk')), parts along dimension 0
The draws below stay inside these ranges and needn't reach their ends.
There are 2 independent parts, one for each index of `grp`. The reference program is written for one: setup_inputs(seed, part) draws one part's arguments, and reference() takes and returns one part's arrays. A program takes and returns all parts, laid end to end along the dimension named above; each array names one. Nothing has to cross between parts.
Inputs may be any that keep to these rules, and one draw needn't show every extreme that they name: `hole_orbitals`: within each determinant the 4 entries are distinct. `particle_orbitals`: within each determinant the 4 entries are distinct.
All inputs are finite; a program needn't handle non-finite values.
Results may differ from the reference program's by a relative error of at most 0.00035.
Values may be sent and summed in bfloat16 or wider, within the bound.
A program may use at most 128 MiB of HBM per device.

```python
import jax
import jax.numpy as jnp
from jax import lax

NOCC = 150
NVIR = 450
NAO = 64
NAV = 64
MAXEXC = 4
WALKERS = 16
DETS = 1024
NCHOL = 512


def distinct_picks(key, columns):
    scores = jax.random.randint(key, (DETS, columns), 0, 1 << 20) * columns + jnp.arange(columns)[None, :]
    return jnp.argsort(scores, axis=1)[:, :MAXEXC].astype(jnp.int32)


def draw_hole_orbitals(key, part):
    return distinct_picks(jax.random.fold_in(key, 11), NAO)


def draw_particle_orbitals(key, part):
    return distinct_picks(jax.random.fold_in(key, 23), NAV)


def draw_greens(key, part):
    first_key = jax.random.fold_in(jax.random.fold_in(key, 37), 0)
    virtual_rows = jnp.arange(NVIR)[:, None]
    occupied_columns = jnp.arange(NOCC)[None, :]
    in_active = (virtual_rows < NAV) & (occupied_columns >= NOCC - NAO)
    scale_map = jnp.where(in_active, 0.5, 0.02).astype(jnp.float32)
    values = jax.random.normal(first_key, (WALKERS, NVIR, NOCC), jnp.float32)
    return jnp.clip(values * scale_map[None, :, :], -2.0, 2.0).astype(jnp.bfloat16)


def set_ends(values, own_key, low, largest):
    shape = values.shape
    place = [jax.random.randint(jax.random.fold_in(own_key, axis), (), 0, shape[axis]) for axis in range(len(shape))]
    values = values.at[tuple(place)].set(low)
    longest = shape.index(max(shape))
    place[longest] = (place[longest] + 1) % shape[longest]
    return values.at[tuple(place)].set(largest)


def level_of(rng, dims, shards, low, high):
    factor_of, own = 1.0, jax.random.fold_in(rng, 6)
    for position, parts in shards:
        draws = jnp.exp(jax.random.uniform(jax.random.fold_in(own, position), (parts,), jnp.float32, low / len(shards), high / len(shards)))
        factor_of = factor_of * jnp.repeat(draws, dims[position] // parts).reshape([-1 if axis == position else 1 for axis in range(len(dims))])
    return factor_of


def normal_values(key, shape, scale, bound, cuts=(), kind=jnp.bfloat16):
    values = scale * jax.random.normal(key, shape, jnp.float32)
    if cuts:
        values = values * level_of(key, shape, cuts, -0.22, 0.18)
    return jnp.clip(values, -bound, bound).astype(kind)


def setup_inputs(seed: int = 0, part: int = 0) -> dict:
    key_list = jax.random.split(jax.random.key(seed), 7)
    own_keys = jax.random.split(jax.random.fold_in(key_list[6], part), 7)
    greens = draw_greens(jax.random.fold_in(jax.random.fold_in(key_list[6], part), 71), part)
    chol_vectors = normal_values(own_keys[1], (NCHOL, NVIR, NOCC), (NVIR * NOCC) ** -0.5, 0.0234375, ((0, 8),))
    hole_orbitals = draw_hole_orbitals(jax.random.fold_in(jax.random.fold_in(key_list[6], part), 71), part)
    particle_orbitals = draw_particle_orbitals(jax.random.fold_in(jax.random.fold_in(key_list[6], part), 71), part)
    excitation_order = set_ends(jax.random.randint(own_keys[4], (DETS,), 0, MAXEXC + 1), jax.random.fold_in(own_keys[4], 1), 0, MAXEXC).astype(jnp.int32)
    amplitudes = normal_values(own_keys[5], (DETS,), 0.1, 0.6, ((0, 8),), jnp.float32)
    return dict(greens=greens, chol_vectors=chol_vectors, hole_orbitals=hole_orbitals, particle_orbitals=particle_orbitals, excitation_order=excitation_order, amplitudes=amplitudes)


def minor_determinant(matrix):
    column_pairs = ((0, 1), (0, 2), (0, 3), (1, 2), (1, 3), (2, 3))
    parity = (1.0, -1.0, 1.0, 1.0, -1.0, 1.0)
    result = 0.0
    for number in range(6):
        first_column, second_column = column_pairs[number]
        third_column, fourth_column = column_pairs[5 - number]
        uppers = matrix[0][first_column] * matrix[1][second_column] - matrix[1][first_column] * matrix[0][second_column]
        lowers = matrix[2][third_column] * matrix[3][fourth_column] - matrix[3][third_column] * matrix[2][fourth_column]
        result = result + parity[number] * uppers * lowers
    return result

def divisor_below(amount, target):
    return max((candidate for candidate in range(1, min(target, amount) + 1) if amount % candidate == 0))

def reference(greens, chol_vectors, hole_orbitals, particle_orbitals, excitation_order, amplitudes):
    offset = NOCC - NAO
    walkers = greens.shape[0]
    active_green = greens[:, :NAV, offset:].astype(jnp.float32)
    det_count = hole_orbitals.shape[0]
    block_size = divisor_below(det_count, 1024)
    blocks = det_count // block_size

    def advance(totals, tables):
        hole_rows, particle_rows, order_rows, weight_rows = tables
        picked = active_green[:, particle_rows[:, :, None], hole_rows[:, None, :]]
        matrix = jnp.transpose(picked, (2, 3, 0, 1))
        positions = jnp.arange(MAXEXC)
        row_live = positions[:, None] < order_rows[None, :]
        live_mask = (row_live[:, None, :] & row_live[None, :, :])[:, :, None, :]
        identity = jnp.eye(MAXEXC, dtype=jnp.float32)[:, :, None, None]
        padded = jnp.where(live_mask, matrix, identity)
        ratios, pullback = jax.vjp(minor_determinant, padded)
        cofactors = pullback(jnp.ones_like(ratios))[0]
        weighted = jnp.where(live_mask, cofactors, 0.0) * weight_rows[None, None, None, :]
        correlation_part = lax.optimization_barrier(jnp.sum(ratios * weight_rows[None, :], axis=1))
        contrib = jnp.transpose(weighted, (2, 3, 0, 1))
        row_index = jnp.broadcast_to(particle_rows[:, :, None], (block_size, MAXEXC, MAXEXC))
        column_index = jnp.broadcast_to(hole_rows[:, None, :], (block_size, MAXEXC, MAXEXC))
        gradient = totals[0].at[:, row_index, column_index].add(contrib)
        return ((gradient, totals[1] + correlation_part), None)
    stacked = (hole_orbitals.reshape(blocks, block_size, MAXEXC), particle_orbitals.reshape(blocks, block_size, MAXEXC), excitation_order.reshape(blocks, block_size), amplitudes.reshape(blocks, block_size))
    zeros = (jnp.zeros((walkers, NAV, NAO), jnp.float32), jnp.zeros((walkers,), jnp.float32))
    (gradient, correlation_sum), _ = lax.scan(advance, zeros, stacked)
    correlation = 1.0 + correlation_sum
    gradient_rows = gradient.reshape(walkers, NAV * NAO).astype(jnp.bfloat16)
    vectors = chol_vectors.shape[0]
    flat_green = greens.reshape(walkers, NVIR * NOCC)
    flat_chol = chol_vectors.reshape(vectors, NVIR * NOCC)
    whole_term = lax.dot_general(flat_green, flat_chol, (((1,), (1,)), ((), ())), preferred_element_type=jnp.float32)
    active_chol = chol_vectors[:, :NAV, offset:].reshape(vectors, NAV * NAO)
    active_term = lax.dot_general(gradient_rows, active_chol, (((1,), (1,)), ((), ())), preferred_element_type=jnp.float32)
    force_bias = correlation[:, None] * whole_term + active_term
    return (correlation, force_bias)
```

```python
import functools

import jax
import jax.numpy as jnp
from jax import lax
from jax.experimental import pallas as pl
from jax.experimental.pallas import tpu as pltpu
from jax.sharding import PartitionSpec as P

NAO = 64
NAV = 64
MAXEXC = 4
BLOCK = 16
CHUNK_BLOCKS = 2
MESH = pl.DeviceIdType.MESH
PAIRS = ((0, 1), (0, 2), (0, 3), (1, 2), (1, 3), (2, 3))
PARITY = (1.0, -1.0, 1.0, 1.0, -1.0, 1.0)


def ratio_and_cofactors(m):
    uppers, lowers = [], []
    for number in range(6):
        a, b = PAIRS[number]
        c, d = PAIRS[5 - number]
        uppers.append(m[0][a] * m[1][b] - m[1][a] * m[0][b])
        lowers.append(m[2][c] * m[3][d] - m[3][c] * m[2][d])
    ratio = 0.0
    cof = [[0.0] * 4 for _ in range(4)]
    for number in range(6):
        a, b = PAIRS[number]
        c, d = PAIRS[5 - number]
        low = PARITY[number] * lowers[number]
        up = PARITY[number] * uppers[number]
        ratio = ratio + low * uppers[number]
        cof[0][a] = cof[0][a] + low * m[1][b]
        cof[1][b] = cof[1][b] + low * m[0][a]
        cof[1][a] = cof[1][a] - low * m[0][b]
        cof[0][b] = cof[0][b] - low * m[1][a]
        cof[2][c] = cof[2][c] + up * m[3][d]
        cof[3][d] = cof[3][d] + up * m[2][c]
        cof[3][c] = cof[3][c] - up * m[2][d]
        cof[2][d] = cof[2][d] - up * m[3][c]
    return ratio, cof


def kernel(
    n, chunks, greens, chol_hbm, holes, particles, order, amp, corr_out, bias_out,
    gbuf, chol, tab, mats, gsend, grecv, gpad, acc, acc2, rsend, rrecv,
    chol_sem, tab_s, tab_r, ring_s, ring_r, grad_s, grad_r, res_s, res_r,
):
    nocc, vectors, nvir = chol_hbm.shape
    dets = tab.shape[-1]
    rows = CHUNK_BLOCKS * BLOCK
    offset = nocc - NAO
    first = offset // BLOCK * BLOCK
    half = n // 2
    me = lax.axis_index("det")

    chol_copies = []
    for c in range(chunks):
        lo, hi = c * rows, min((c + 1) * rows, nocc)
        copy = pltpu.make_async_copy(
            chol_hbm.at[pl.ds(lo, hi - lo)], chol.at[pl.ds(lo, hi - lo)], chol_sem.at[c]
        )
        copy.start()
        chol_copies.append(copy)

    own_table = jnp.concatenate(
        [
            holes[...].astype(jnp.float32),
            particles[...].astype(jnp.float32),
            order[...].astype(jnp.float32),
            amp[...],
            jnp.zeros((6, dets), jnp.float32),
        ],
        axis=0,
    )
    tab[me] = own_table
    gbuf[me] = jnp.zeros(gbuf.shape[1:], jnp.bfloat16)
    gbuf[me, 0:nocc, 0:nvir] = greens[0]

    barrier = pltpu.get_barrier_semaphore()
    for k in range(1, n):
        pl.semaphore_signal(
            barrier, inc=1, device_id={"det": lax.rem(me + k, n)}, device_id_type=MESH
        )
    pl.semaphore_wait(barrier, n - 1)

    def all_to_peers(source, target, send, recv, pick):
        copies = []
        for k in range(1, n):
            peer = lax.rem(me + k, n)
            copy = pltpu.make_async_remote_copy(
                src_ref=source.at[pick(peer)],
                dst_ref=target.at[me],
                send_sem=send.at[k],
                recv_sem=recv.at[k],
                device_id={"det": peer},
                device_id_type=MESH,
            )
            copy.start()
            copies.append(copy)
        return copies

    tab_copies = all_to_peers(tab, tab, tab_s, tab_r, lambda peer: me)

    def det_of(position):
        position = lax.rem(position + 2 * n, n)
        return jnp.where(position < half, 2 * position, 2 * (n - 1 - position) + 1)

    even = lax.rem(me, 2) == 0
    position = jnp.where(even, me // 2, n - 1 - me // 2)
    neighbour = (det_of(position + 1), det_of(position - 1))
    step = (1, -1)

    def hops(way, c):
        return half if (way == 0) == (c % 2 == 0) else n - 1 - half

    def ring_copy(way, hop, c):
        slot = det_of(position - step[way] * (hop - 1))
        piece = gbuf.at[slot, pl.ds(c * rows, rows)]
        return pltpu.make_async_remote_copy(
            src_ref=piece,
            dst_ref=piece,
            send_sem=ring_s.at[way, hop - 1, c],
            recv_sem=ring_r.at[way, hop - 1, c],
            device_id={"det": neighbour[way]},
            device_id_type=MESH,
        )

    ring_copies = {}

    def send_on(way, hop, c):
        if hop <= hops(way, c):
            copy = ring_copy(way, hop, c)
            copy.start()
            ring_copies[way, hop, c] = copy

    def relay(hop, c):
        for way in range(2):
            if hop <= hops(way, c):
                ring_copies[way, hop, c].wait_recv()
                send_on(way, hop + 1, c)

    for c in range(chunks):
        for way in range(2):
            send_on(way, 1, c)

    active = greens[0, first:nocc, 0:128].astype(jnp.float32)[
        offset - first:, 0:NAV
    ].astype(jnp.bfloat16)
    lanes_i = lax.broadcasted_iota(jnp.int32, (NAO, dets), 0).astype(jnp.float32)

    for copy in tab_copies:
        copy.wait_recv()

    def particle_hot(s):
        return jnp.concatenate(
            [
                (tab[s, MAXEXC + j:MAXEXC + j + 1, :] == lanes_i)
                .astype(jnp.float32)
                .astype(jnp.bfloat16)
                for j in range(MAXEXC)
            ],
            axis=1,
        )

    for s in range(n):
        picked = jnp.dot(active, particle_hot(s), preferred_element_type=jnp.float32)
        for l in range(MAXEXC):
            chosen = tab[s, l:l + 1, :] == lanes_i
            for j in range(MAXEXC):
                value = jnp.where(chosen, picked[:, j * dets:(j + 1) * dets], 0.0)
                mats[j * MAXEXC + l, s:s + 1, :] = jnp.sum(value, axis=0, keepdims=True)

    for c in range(chunks):
        relay(1, c)

    orders = tab[:, 2 * MAXEXC, :]
    weights = tab[:, 2 * MAXEXC + 1, :]
    live = [orders > float(j) for j in range(MAXEXC)]
    matrix = [
        [
            jnp.where(live[max(j, l)], mats[j * MAXEXC + l], 1.0 if j == l else 0.0)
            for l in range(MAXEXC)
        ]
        for j in range(MAXEXC)
    ]
    ratio, cofactors = ratio_and_cofactors(matrix)
    corr = 1.0 + jnp.sum(ratio * weights, keepdims=True)
    for j in range(MAXEXC):
        for l in range(MAXEXC):
            mats[j * MAXEXC + l] = jnp.where(
                live[max(j, l)], cofactors[j][l] * weights, 0.0
            )

    gradient = jnp.zeros((2 * NAO, NAV), jnp.float32)
    for s in range(n):
        chosen = [tab[s, l:l + 1, :] == lanes_i for l in range(MAXEXC)]
        spread = []
        for j in range(MAXEXC):
            total = jnp.zeros((NAO, dets), jnp.float32)
            for l in range(MAXEXC):
                total = jnp.where(
                    chosen[l], mats[j * MAXEXC + l, s:s + 1, :], total
                )
            upper = total.astype(jnp.bfloat16)
            lower = (total - upper.astype(jnp.float32)).astype(jnp.bfloat16)
            spread.append(jnp.concatenate([upper, lower], axis=0))
        gradient = gradient + lax.dot_general(
            jnp.concatenate(spread, axis=1),
            particle_hot(s),
            (((1,), (1,)), ((), ())),
            preferred_element_type=jnp.float32,
        )
    gradient = gradient[:NAO] + gradient[NAO:]
    packed = jnp.concatenate([gradient[:NAO // 2], gradient[NAO // 2:]], axis=1)
    gsend[...] = packed.astype(jnp.bfloat16)
    grecv[me] = packed.astype(jnp.bfloat16)

    grad_copies = []
    for k in range(1, n):
        copy = pltpu.make_async_remote_copy(
            src_ref=gsend,
            dst_ref=grecv.at[me],
            send_sem=grad_s.at[k],
            recv_sem=grad_r.at[k],
            device_id={"det": lax.rem(me + k, n)},
            device_id_type=MESH,
        )
        copy.start()
        grad_copies.append(copy)

    for hop in range(2, half):
        for c in range(chunks):
            relay(hop, c)

    acc[...] = jnp.zeros_like(acc)
    acc2[...] = jnp.zeros_like(acc2)
    gpad[...] = jnp.zeros_like(gpad)

    def add_block(target, start, right, depth):
        count = min(BLOCK, nocc - start)
        left = chol[start:start + count, :, 0:depth].reshape(count * vectors, depth)
        target[0:count * vectors, :] += lax.dot_general(
            left, right, (((1,), (1,)), ((), ())), preferred_element_type=jnp.float32
        )

    def finish(c):
        if half > 1:
            relay(half, c)
        chol_copies[c].wait()
        for start in range(c * rows, min((c + 1) * rows, nocc), BLOCK):
            right = gbuf[:, start:start + BLOCK, :].reshape(n * BLOCK, gbuf.shape[2])
            add_block(acc, start, right[:, 0:nvir], nvir)

    for c in range(chunks - 1):
        finish(c)
    for copy in grad_copies:
        copy.wait_recv()
    chol_copies[chunks - 1].wait()
    low = offset - first
    for s in range(n):
        value = grecv[s].astype(jnp.float32)
        gpad[s, low:low + NAO // 2, 0:NAV] = value[:, 0:NAV]
        gpad[s, low + NAO // 2:low + NAO, 0:NAV] = value[:, NAV:]
    for start in range(first, nocc, BLOCK):
        right = gpad[:, start - first:start - first + BLOCK, :].astype(jnp.bfloat16)
        add_block(acc2, start, right.reshape(n * BLOCK, 128)[:, 0:NAV], NAV)

    columns = n * BLOCK
    column_of = lax.broadcasted_iota(jnp.int32, (vectors, columns), 1)
    sel_w = lax.broadcasted_iota(jnp.int32, (n, columns), 0)
    sel_c = lax.broadcasted_iota(jnp.int32, (n, columns), 1)
    selector = jnp.where(sel_c // BLOCK == sel_w, 1.0, 0.0)

    def diagonal(target):
        total = jnp.zeros((vectors, columns), jnp.float32)
        for i in range(BLOCK):
            total = total + jnp.where(
                column_of % BLOCK == i, target[i * vectors:(i + 1) * vectors, :], 0.0
            )
        return lax.dot_general(
            selector,
            total,
            (((1,), (1,)), ((), ())),
            precision=lax.Precision.HIGHEST,
            preferred_element_type=jnp.float32,
        )

    active_part = diagonal(acc2)
    relay_last = chunks - 1
    if half > 1:
        relay(half, relay_last)
    for start in range(relay_last * rows, nocc, BLOCK):
        right = gbuf[:, start:start + BLOCK, :].reshape(n * BLOCK, gbuf.shape[2])
        add_block(acc, start, right[:, 0:nvir], nvir)
    whole_part = diagonal(acc)
    both = jnp.concatenate([whole_part, active_part], axis=1)
    for w in range(n):
        rsend[w] = both[w:w + 1, :]
    rrecv[me] = rsend[me]
    res_copies = all_to_peers(rsend, rrecv, res_s, res_r, lambda peer: peer)
    corr_out[0] = corr[0, 0]
    for copy in res_copies:
        copy.wait_recv()
    for s in range(n):
        value = rrecv[s]
        bias_out[0:1, s * vectors:(s + 1) * vectors] = (
            corr * value[:, 0:vectors] + value[:, vectors:]
        )
    for copies in (tab_copies, grad_copies, res_copies, ring_copies.values()):
        for copy in copies:
            copy.wait_send()


def solution(mesh):
    n = mesh.shape["det"]

    def shards(greens, chol_vectors, holes, particles, order, amplitudes):
        vectors, nvir, nocc = chol_vectors.shape
        dets = holes.shape[0]
        rows = CHUNK_BLOCKS * BLOCK
        chunks = -(-nocc // rows)
        lanes = -(-nvir // 128) * 128
        first = (nocc - NAO) // BLOCK * BLOCK
        pad_rows = -(-(nocc - first) // BLOCK) * BLOCK
        half = max(1, n // 2)
        vmem = pl.BlockSpec(memory_space=pltpu.VMEM)
        dma = pltpu.SemaphoreType.DMA
        return pl.pallas_call(
            functools.partial(kernel, n, chunks),
            out_shape=(
                jax.ShapeDtypeStruct((1,), jnp.float32),
                jax.ShapeDtypeStruct((1, n * vectors), jnp.float32),
            ),
            in_specs=[vmem, pl.BlockSpec(memory_space=pl.ANY)] + [vmem] * 4,
            out_specs=(pl.BlockSpec(memory_space=pltpu.SMEM), vmem),
            scratch_shapes=[
                pltpu.VMEM((n, chunks * rows, lanes), jnp.bfloat16),
                pltpu.VMEM((nocc, vectors, nvir), jnp.bfloat16),
                pltpu.VMEM((n, 16, dets), jnp.float32),
                pltpu.VMEM((MAXEXC * MAXEXC, n, dets), jnp.float32),
                pltpu.VMEM((NAO // 2, 2 * NAV), jnp.bfloat16),
                pltpu.VMEM((n, NAO // 2, 2 * NAV), jnp.bfloat16),
                pltpu.VMEM((n, pad_rows, 128), jnp.float32),
                pltpu.VMEM((BLOCK * vectors, n * BLOCK), jnp.float32),
                pltpu.VMEM((BLOCK * vectors, n * BLOCK), jnp.float32),
                pltpu.VMEM((n, 1, 2 * vectors), jnp.float32),
                pltpu.VMEM((n, 1, 2 * vectors), jnp.float32),
                dma((chunks,)),
                dma((n,)),
                dma((n,)),
                dma((2, half, chunks)),
                dma((2, half, chunks)),
                dma((n,)),
                dma((n,)),
                dma((n,)),
                dma((n,)),
            ],
            compiler_params=pltpu.CompilerParams(
                collective_id=0, has_side_effects=True
            ),
        )(
            jnp.transpose(greens, (0, 2, 1)),
            jnp.transpose(chol_vectors, (2, 0, 1)),
            holes.T,
            particles.T,
            order.reshape(1, dets),
            amplitudes.reshape(1, dets),
        )

    placed = (
        P(("grp", "det", "wlk"), None, None),
        P(("grp", "det"), None, None),
        P(("grp", "det"), None),
        P(("grp", "det"), None),
        P(("grp", "det")),
        P(("grp", "det")),
    )
    return jax.shard_map(
        shards,
        mesh=mesh,
        in_specs=placed,
        out_specs=(P(("grp", "det", "wlk")), P(("grp", "det", "wlk"), None)),
        check_vma=False,
    )
```

```python
import functools

import jax
import jax.numpy as jnp
from jax import lax
from jax.experimental import pallas as pl
from jax.experimental.pallas import tpu as pltpu
from jax.sharding import PartitionSpec as P

NAO = 64
NAV = 64
MAXEXC = 4
BLOCK = 16
CHUNK_BLOCKS = 2
EARLY = 3
MESH = pl.DeviceIdType.MESH
PAIRS = ((0, 1), (0, 2), (0, 3), (1, 2), (1, 3), (2, 3))
PARITY = (1.0, -1.0, 1.0, 1.0, -1.0, 1.0)


def ratio_and_cofactors(m):
    uppers, lowers = [], []
    for number in range(6):
        a, b = PAIRS[number]
        c, d = PAIRS[5 - number]
        uppers.append(m[0][a] * m[1][b] - m[1][a] * m[0][b])
        lowers.append(m[2][c] * m[3][d] - m[3][c] * m[2][d])
    ratio = 0.0
    cof = [[0.0] * 4 for _ in range(4)]
    for number in range(6):
        a, b = PAIRS[number]
        c, d = PAIRS[5 - number]
        low = PARITY[number] * lowers[number]
        up = PARITY[number] * uppers[number]
        ratio = ratio + low * uppers[number]
        cof[0][a] = cof[0][a] + low * m[1][b]
        cof[1][b] = cof[1][b] + low * m[0][a]
        cof[1][a] = cof[1][a] - low * m[0][b]
        cof[0][b] = cof[0][b] - low * m[1][a]
        cof[2][c] = cof[2][c] + up * m[3][d]
        cof[3][d] = cof[3][d] + up * m[2][c]
        cof[3][c] = cof[3][c] - up * m[2][d]
        cof[2][d] = cof[2][d] - up * m[3][c]
    return ratio, cof


def kernel(
    n, chunks, greens, chol_hbm, holes, particles, order, amp, corr_out, bias_out,
    gbuf, chol, tab_wire, tab, mats, gsend, grecv, gpad, acc, acc2, rsend, rrecv,
    chol_sem, tab_s, tab_r, ring_s, ring_r, grad_s, grad_r, res_s, res_r,
):
    nocc, vectors, nvir = chol_hbm.shape
    dets = tab.shape[-1]
    rows = CHUNK_BLOCKS * BLOCK
    offset = nocc - NAO
    first = offset // BLOCK * BLOCK
    half = n // 2
    me = lax.axis_index("det")

    barrier = pltpu.get_barrier_semaphore()
    for k in range(1, n):
        pl.semaphore_signal(
            barrier, inc=1, device_id={"det": lax.rem(me + k, n)}, device_id_type=MESH
        )

    chol_copies = []
    for c in range(chunks):
        lo, hi = c * rows, min((c + 1) * rows, nocc)
        copy = pltpu.make_async_copy(
            chol_hbm.at[pl.ds(lo, hi - lo)], chol.at[pl.ds(lo, hi - lo)], chol_sem.at[c]
        )
        copy.start()
        chol_copies.append(copy)

    def piece_of(value):
        return value.astype(jnp.bfloat16).astype(jnp.float32)

    amp_high = piece_of(amp[...])
    amp_mid = piece_of(amp[...] - amp_high)
    amp_low = amp[...] - amp_high - amp_mid
    own_table = jnp.concatenate(
        [
            holes[...].astype(jnp.float32),
            particles[...].astype(jnp.float32),
            order[...].astype(jnp.float32),
            amp_high,
            amp_mid,
            amp_low,
            jnp.zeros((4, dets), jnp.float32),
        ],
        axis=0,
    )
    tab_wire[me] = own_table.astype(jnp.bfloat16)
    gbuf[me] = jnp.zeros(gbuf.shape[1:], jnp.bfloat16)
    gbuf[me, 0:nocc, 0:nvir] = greens[0]

    pl.semaphore_wait(barrier, n - 1)

    def all_to_peers(source, target, send, recv, pick):
        copies = []
        for k in range(1, n):
            peer = lax.rem(me + k, n)
            copy = pltpu.make_async_remote_copy(
                src_ref=source.at[pick(peer)],
                dst_ref=target.at[me],
                send_sem=send.at[k],
                recv_sem=recv.at[k],
                device_id={"det": peer},
                device_id_type=MESH,
            )
            copy.start()
            copies.append(copy)
        return copies

    tab_copies = all_to_peers(tab_wire, tab_wire, tab_s, tab_r, lambda peer: me)

    def det_of(position):
        position = lax.rem(position + 2 * n, n)
        return jnp.where(position < half, 2 * position, 2 * (n - 1 - position) + 1)

    even = lax.rem(me, 2) == 0
    position = jnp.where(even, me // 2, n - 1 - me // 2)
    neighbour = (det_of(position + 1), det_of(position - 1))
    step = (1, -1)

    def hops(way, c):
        return half if (way == 0) == (c % 2 == 0) else n - 1 - half

    def ring_copy(way, hop, c):
        slot = det_of(position - step[way] * (hop - 1))
        count = min(rows, -(-(nocc - c * rows) // 8) * 8)
        piece = gbuf.at[slot, pl.ds(c * rows, count)]
        return pltpu.make_async_remote_copy(
            src_ref=piece,
            dst_ref=piece,
            send_sem=ring_s.at[way, hop - 1, c],
            recv_sem=ring_r.at[way, hop - 1, c],
            device_id={"det": neighbour[way]},
            device_id_type=MESH,
        )

    ring_copies = {}

    def send_on(way, hop, c):
        if hop <= hops(way, c):
            copy = ring_copy(way, hop, c)
            copy.start()
            ring_copies[way, hop, c] = copy

    def relay(hop, c):
        for way in range(2):
            if hop <= hops(way, c):
                ring_copies[way, hop, c].wait_recv()
                send_on(way, hop + 1, c)

    for c in range(chunks):
        for way in range(2):
            send_on(way, 1, c)

    active = greens[0, first:nocc, 0:128].astype(jnp.float32)[
        offset - first:, 0:NAV
    ].astype(jnp.bfloat16)
    lanes_i = lax.broadcasted_iota(jnp.int32, (NAO, dets), 0).astype(jnp.float32)

    for c in range(min(EARLY, chunks)):
        relay(1, c)
    for copy in tab_copies:
        copy.wait_recv()
    for s in range(n):
        tab[s] = tab_wire[s].astype(jnp.float32)

    def particle_hot(s):
        return jnp.concatenate(
            [
                (tab[s, MAXEXC + j:MAXEXC + j + 1, :] == lanes_i)
                .astype(jnp.float32)
                .astype(jnp.bfloat16)
                for j in range(MAXEXC)
            ],
            axis=1,
        )

    for s in range(n):
        picked = jnp.dot(active, particle_hot(s), preferred_element_type=jnp.float32)
        for l in range(MAXEXC):
            chosen = tab[s, l:l + 1, :] == lanes_i
            for j in range(MAXEXC):
                value = jnp.where(chosen, picked[:, j * dets:(j + 1) * dets], 0.0)
                mats[j * MAXEXC + l, s:s + 1, :] = jnp.sum(value, axis=0, keepdims=True)

    for c in range(EARLY, chunks):
        relay(1, c)

    orders = tab[:, 2 * MAXEXC, :]
    weights = tab[:, 2 * MAXEXC + 1, :] + tab[:, 2 * MAXEXC + 2, :]
    weights = weights + tab[:, 2 * MAXEXC + 3, :]
    live = [orders > float(j) for j in range(MAXEXC)]
    matrix = [
        [
            jnp.where(live[max(j, l)], mats[j * MAXEXC + l], 1.0 if j == l else 0.0)
            for l in range(MAXEXC)
        ]
        for j in range(MAXEXC)
    ]
    ratio, cofactors = ratio_and_cofactors(matrix)
    corr = 1.0 + jnp.sum(ratio * weights, keepdims=True)
    for j in range(MAXEXC):
        for l in range(MAXEXC):
            mats[j * MAXEXC + l] = jnp.where(
                live[max(j, l)], cofactors[j][l] * weights, 0.0
            )

    gradient = jnp.zeros((2 * NAO, NAV), jnp.float32)
    for s in range(n):
        chosen = [tab[s, l:l + 1, :] == lanes_i for l in range(MAXEXC)]
        spread = []
        for j in range(MAXEXC):
            total = jnp.zeros((NAO, dets), jnp.float32)
            for l in range(MAXEXC):
                total = jnp.where(
                    chosen[l], mats[j * MAXEXC + l, s:s + 1, :], total
                )
            upper = total.astype(jnp.bfloat16)
            lower = (total - upper.astype(jnp.float32)).astype(jnp.bfloat16)
            spread.append(jnp.concatenate([upper, lower], axis=0))
        gradient = gradient + lax.dot_general(
            jnp.concatenate(spread, axis=1),
            particle_hot(s),
            (((1,), (1,)), ((), ())),
            preferred_element_type=jnp.float32,
        )
    gradient = gradient[:NAO] + gradient[NAO:]
    packed = jnp.concatenate([gradient[:NAO // 2], gradient[NAO // 2:]], axis=1)
    gsend[...] = packed.astype(jnp.bfloat16)
    grecv[me] = packed.astype(jnp.bfloat16)

    grad_copies = []
    for k in range(1, n):
        copy = pltpu.make_async_remote_copy(
            src_ref=gsend,
            dst_ref=grecv.at[me],
            send_sem=grad_s.at[k],
            recv_sem=grad_r.at[k],
            device_id={"det": lax.rem(me + k, n)},
            device_id_type=MESH,
        )
        copy.start()
        grad_copies.append(copy)

    for hop in range(2, half):
        for c in range(chunks):
            relay(hop, c)

    acc[...] = jnp.zeros_like(acc)
    acc2[...] = jnp.zeros_like(acc2)
    gpad[...] = jnp.zeros_like(gpad)

    def add_block(target, start, right, depth):
        count = min(BLOCK, nocc - start)
        left = chol[start:start + count, :, 0:depth].reshape(count * vectors, depth)
        target[0:count * vectors, :] += lax.dot_general(
            left, right, (((1,), (1,)), ((), ())), preferred_element_type=jnp.float32
        )

    def finish(c):
        if half > 1:
            relay(half, c)
        chol_copies[c].wait()
        for start in range(c * rows, min((c + 1) * rows, nocc), BLOCK):
            right = gbuf[:, start:start + BLOCK, :].reshape(n * BLOCK, gbuf.shape[2])
            add_block(acc, start, right[:, 0:nvir], nvir)

    for c in range(chunks - 1):
        finish(c)
    for copy in grad_copies:
        copy.wait_recv()
    chol_copies[chunks - 1].wait()
    low = offset - first
    for s in range(n):
        value = grecv[s].astype(jnp.float32)
        gpad[s, low:low + NAO // 2, 0:NAV] = value[:, 0:NAV]
        gpad[s, low + NAO // 2:low + NAO, 0:NAV] = value[:, NAV:]
    for start in range(first, nocc, BLOCK):
        right = gpad[:, start - first:start - first + BLOCK, :].astype(jnp.bfloat16)
        add_block(acc2, start, right.reshape(n * BLOCK, 128)[:, 0:NAV], NAV)

    columns = n * BLOCK
    column_of = lax.broadcasted_iota(jnp.int32, (vectors, columns), 1)
    sel_w = lax.broadcasted_iota(jnp.int32, (n, columns), 0)
    sel_c = lax.broadcasted_iota(jnp.int32, (n, columns), 1)
    selector = jnp.where(sel_c // BLOCK == sel_w, 1.0, 0.0)

    def diagonal(target):
        total = jnp.zeros((vectors, columns), jnp.float32)
        for i in range(BLOCK):
            total = total + jnp.where(
                column_of % BLOCK == i, target[i * vectors:(i + 1) * vectors, :], 0.0
            )
        return lax.dot_general(
            selector,
            total,
            (((1,), (1,)), ((), ())),
            precision=lax.Precision.HIGHEST,
            preferred_element_type=jnp.float32,
        )

    active_part = diagonal(acc2)
    relay_last = chunks - 1
    if half > 1:
        relay(half, relay_last)
    for start in range(relay_last * rows, nocc, BLOCK):
        right = gbuf[:, start:start + BLOCK, :].reshape(n * BLOCK, gbuf.shape[2])
        add_block(acc, start, right[:, 0:nvir], nvir)
    whole_part = diagonal(acc)
    both = jnp.concatenate([whole_part, active_part], axis=1)
    for w in range(n):
        rsend[w] = both[w:w + 1, :]
    rrecv[me] = rsend[me]
    res_copies = all_to_peers(rsend, rrecv, res_s, res_r, lambda peer: peer)
    corr_out[0] = corr[0, 0]
    for copy in res_copies:
        copy.wait_recv()
    for s in range(n):
        value = rrecv[s]
        bias_out[0:1, s * vectors:(s + 1) * vectors] = (
            corr * value[:, 0:vectors] + value[:, vectors:]
        )
    for copies in (tab_copies, grad_copies, res_copies, ring_copies.values()):
        for copy in copies:
            copy.wait_send()


def solution(mesh):
    n = mesh.shape["det"]

    def shards(greens, chol_vectors, holes, particles, order, amplitudes):
        vectors, nvir, nocc = chol_vectors.shape
        dets = holes.shape[0]
        rows = CHUNK_BLOCKS * BLOCK
        chunks = -(-nocc // rows)
        lanes = -(-nvir // 128) * 128
        first = (nocc - NAO) // BLOCK * BLOCK
        pad_rows = -(-(nocc - first) // BLOCK) * BLOCK
        half = max(1, n // 2)
        vmem = pl.BlockSpec(memory_space=pltpu.VMEM)
        dma = pltpu.SemaphoreType.DMA
        return pl.pallas_call(
            functools.partial(kernel, n, chunks),
            out_shape=(
                jax.ShapeDtypeStruct((1,), jnp.float32),
                jax.ShapeDtypeStruct((1, n * vectors), jnp.float32),
            ),
            in_specs=[vmem, pl.BlockSpec(memory_space=pl.ANY)] + [vmem] * 4,
            out_specs=(pl.BlockSpec(memory_space=pltpu.SMEM), vmem),
            scratch_shapes=[
                pltpu.VMEM((n, chunks * rows, lanes), jnp.bfloat16),
                pltpu.VMEM((nocc, vectors, nvir), jnp.bfloat16),
                pltpu.VMEM((n, 16, dets), jnp.bfloat16),
                pltpu.VMEM((n, 16, dets), jnp.float32),
                pltpu.VMEM((MAXEXC * MAXEXC, n, dets), jnp.float32),
                pltpu.VMEM((NAO // 2, 2 * NAV), jnp.bfloat16),
                pltpu.VMEM((n, NAO // 2, 2 * NAV), jnp.bfloat16),
                pltpu.VMEM((n, pad_rows, 128), jnp.float32),
                pltpu.VMEM((BLOCK * vectors, n * BLOCK), jnp.float32),
                pltpu.VMEM((BLOCK * vectors, n * BLOCK), jnp.float32),
                pltpu.VMEM((n, 1, 2 * vectors), jnp.float32),
                pltpu.VMEM((n, 1, 2 * vectors), jnp.float32),
                dma((chunks,)),
                dma((n,)),
                dma((n,)),
                dma((2, half, chunks)),
                dma((2, half, chunks)),
                dma((n,)),
                dma((n,)),
                dma((n,)),
                dma((n,)),
            ],
            compiler_params=pltpu.CompilerParams(
                collective_id=0, has_side_effects=True
            ),
        )(
            jnp.transpose(greens, (0, 2, 1)),
            jnp.transpose(chol_vectors, (2, 0, 1)),
            holes.T,
            particles.T,
            order.reshape(1, dets),
            amplitudes.reshape(1, dets),
        )

    placed = (
        P(("grp", "det", "wlk"), None, None),
        P(("grp", "det"), None, None),
        P(("grp", "det"), None),
        P(("grp", "det"), None),
        P(("grp", "det")),
        P(("grp", "det")),
    )
    return jax.shard_map(
        shards,
        mesh=mesh,
        in_specs=placed,
        out_specs=(P(("grp", "det", "wlk")), P(("grp", "det", "wlk"), None)),
        check_vma=False,
    )
```

```python
import functools

import jax
import jax.numpy as jnp
from jax import lax
from jax.experimental import pallas as pl
from jax.experimental.pallas import tpu as pltpu
from jax.sharding import PartitionSpec as P

NAO = 64
NAV = 64
MAXEXC = 4
BLOCK = 16
CHUNK_BLOCKS = 2
SKEW = 0.4
MINORS_AT = 1.7
GRADIENT_AT = 2.5
ACTIVE_AFTER = 0.3
MESH = pl.DeviceIdType.MESH
PAIRS = ((0, 1), (0, 2), (0, 3), (1, 2), (1, 3), (2, 3))
PARITY = (1.0, -1.0, 1.0, 1.0, -1.0, 1.0)


def ratio_and_cofactors(m):
    uppers, lowers = [], []
    for number in range(6):
        a, b = PAIRS[number]
        c, d = PAIRS[5 - number]
        uppers.append(m[0][a] * m[1][b] - m[1][a] * m[0][b])
        lowers.append(m[2][c] * m[3][d] - m[3][c] * m[2][d])
    ratio = 0.0
    cof = [[0.0] * 4 for _ in range(4)]
    for number in range(6):
        a, b = PAIRS[number]
        c, d = PAIRS[5 - number]
        low = PARITY[number] * lowers[number]
        up = PARITY[number] * uppers[number]
        ratio = ratio + low * uppers[number]
        cof[0][a] = cof[0][a] + low * m[1][b]
        cof[1][b] = cof[1][b] + low * m[0][a]
        cof[1][a] = cof[1][a] - low * m[0][b]
        cof[0][b] = cof[0][b] - low * m[1][a]
        cof[2][c] = cof[2][c] + up * m[3][d]
        cof[3][d] = cof[3][d] + up * m[2][c]
        cof[3][c] = cof[3][c] - up * m[2][d]
        cof[2][d] = cof[2][d] - up * m[3][c]
    return ratio, cof


def kernel(
    n, chunks, greens, chol_hbm, holes, particles, order, amp, corr_out, bias_out,
    gbuf, chol, tab_wire, tab, mats, gsend, grecv, gpad, acc, acc2, rsend, rrecv,
    chol_sem, tab_s, tab_r, ring_s, ring_r, grad_s, grad_r, res_s, res_r,
):
    nocc, vectors, nvir = chol_hbm.shape
    dets = tab.shape[-1]
    rows = CHUNK_BLOCKS * BLOCK
    offset = nocc - NAO
    first = offset // BLOCK * BLOCK
    half = n // 2
    me = lax.axis_index("det")

    barrier = pltpu.get_barrier_semaphore()
    for k in range(1, n):
        pl.semaphore_signal(
            barrier, inc=1, device_id={"det": lax.rem(me + k, n)}, device_id_type=MESH
        )

    chol_copies = []
    for c in range(chunks):
        lo, hi = c * rows, min((c + 1) * rows, nocc)
        copy = pltpu.make_async_copy(
            chol_hbm.at[pl.ds(lo, hi - lo)], chol.at[pl.ds(lo, hi - lo)], chol_sem.at[c]
        )
        copy.start()
        chol_copies.append(copy)

    def piece_of(value):
        return value.astype(jnp.bfloat16).astype(jnp.float32)

    amp_high = piece_of(amp[...])
    amp_mid = piece_of(amp[...] - amp_high)
    amp_low = amp[...] - amp_high - amp_mid
    own_table = jnp.concatenate(
        [
            holes[...].astype(jnp.float32),
            particles[...].astype(jnp.float32),
            order[...].astype(jnp.float32),
            amp_high,
            amp_mid,
            amp_low,
            jnp.zeros((4, dets), jnp.float32),
        ],
        axis=0,
    )
    tab_wire[me] = own_table.astype(jnp.bfloat16)
    gbuf[me] = jnp.zeros(gbuf.shape[1:], jnp.bfloat16)
    gbuf[me, 0:nocc, 0:nvir] = greens[0]

    pl.semaphore_wait(barrier, n - 1)

    def all_to_peers(source, target, send, recv, pick):
        copies = []
        for k in range(1, n):
            peer = lax.rem(me + k, n)
            copy = pltpu.make_async_remote_copy(
                src_ref=source.at[pick(peer)],
                dst_ref=target.at[me],
                send_sem=send.at[k],
                recv_sem=recv.at[k],
                device_id={"det": peer},
                device_id_type=MESH,
            )
            copy.start()
            copies.append(copy)
        return copies

    tab_copies = all_to_peers(tab_wire, tab_wire, tab_s, tab_r, lambda peer: me)

    def det_of(position):
        position = lax.rem(position + 2 * n, n)
        return jnp.where(position < half, 2 * position, 2 * (n - 1 - position) + 1)

    even = lax.rem(me, 2) == 0
    position = jnp.where(even, me // 2, n - 1 - me // 2)
    neighbour = (det_of(position + 1), det_of(position - 1))
    step = (1, -1)

    def hops(way, c):
        return half if (way == 0) == (c % 2 == 0) else n - 1 - half

    def ring_copy(way, hop, c):
        slot = det_of(position - step[way] * (hop - 1))
        count = min(rows, -(-(nocc - c * rows) // 8) * 8)
        piece = gbuf.at[slot, pl.ds(c * rows, count)]
        return pltpu.make_async_remote_copy(
            src_ref=piece,
            dst_ref=piece,
            send_sem=ring_s.at[way, hop - 1, c],
            recv_sem=ring_r.at[way, hop - 1, c],
            device_id={"det": neighbour[way]},
            device_id_type=MESH,
        )

    ring_copies = {}

    def send_on(way, hop, c):
        if hop <= hops(way, c):
            copy = ring_copy(way, hop, c)
            copy.start()
            ring_copies[way, hop, c] = copy

    def relay(hop, c):
        for way in range(2):
            if hop <= hops(way, c):
                ring_copies[way, hop, c].wait_recv()
                send_on(way, hop + 1, c)

    active = greens[0, first:nocc, 0:128].astype(jnp.float32)[
        offset - first:, 0:NAV
    ].astype(jnp.bfloat16)
    lanes_i = lax.broadcasted_iota(jnp.int32, (NAO, dets), 0).astype(jnp.float32)

    def particle_hot(s):
        return jnp.concatenate(
            [
                (tab[s, MAXEXC + j:MAXEXC + j + 1, :] == lanes_i)
                .astype(jnp.float32)
                .astype(jnp.bfloat16)
                for j in range(MAXEXC)
            ],
            axis=1,
        )

    def add_block(target, start, right, depth):
        count = min(BLOCK, nocc - start)
        left = chol[start:start + count, :, 0:depth].reshape(count * vectors, depth)
        target[0:count * vectors, :] += lax.dot_general(
            left, right, (((1,), (1,)), ((), ())), preferred_element_type=jnp.float32
        )

    columns = n * BLOCK
    column_of = lax.broadcasted_iota(jnp.int32, (vectors, columns), 1)
    sel_w = lax.broadcasted_iota(jnp.int32, (n, columns), 0)
    sel_c = lax.broadcasted_iota(jnp.int32, (n, columns), 1)
    selector = jnp.where(sel_c // BLOCK == sel_w, 1.0, 0.0)

    def diagonal(target):
        total = jnp.zeros((vectors, columns), jnp.float32)
        for i in range(BLOCK):
            total = total + jnp.where(
                column_of % BLOCK == i, target[i * vectors:(i + 1) * vectors, :], 0.0
            )
        return lax.dot_general(
            selector,
            total,
            (((1,), (1,)), ((), ())),
            precision=lax.Precision.HIGHEST,
            preferred_element_type=jnp.float32,
        )

    state = {}

    def begin(c):
        for way in range(2):
            send_on(way, 1, c)

    def pick_minors():
        for copy in tab_copies:
            copy.wait_recv()
        for s in range(n):
            tab[s] = tab_wire[s].astype(jnp.float32)

        for s in range(n):
            picked = jnp.dot(active, particle_hot(s), preferred_element_type=jnp.float32)
            for l in range(MAXEXC):
                chosen = tab[s, l:l + 1, :] == lanes_i
                for j in range(MAXEXC):
                    value = jnp.where(chosen, picked[:, j * dets:(j + 1) * dets], 0.0)
                    mats[j * MAXEXC + l, s:s + 1, :] = jnp.sum(value, axis=0, keepdims=True)

    def differentiate():
        orders = tab[:, 2 * MAXEXC, :]
        weights = tab[:, 2 * MAXEXC + 1, :] + tab[:, 2 * MAXEXC + 2, :]
        weights = weights + tab[:, 2 * MAXEXC + 3, :]
        live = [orders > float(j) for j in range(MAXEXC)]
        matrix = [
            [
                jnp.where(live[max(j, l)], mats[j * MAXEXC + l], 1.0 if j == l else 0.0)
                for l in range(MAXEXC)
            ]
            for j in range(MAXEXC)
        ]
        ratio, cofactors = ratio_and_cofactors(matrix)
        corr = 1.0 + jnp.sum(ratio * weights, keepdims=True)
        for j in range(MAXEXC):
            for l in range(MAXEXC):
                mats[j * MAXEXC + l] = jnp.where(
                    live[max(j, l)], cofactors[j][l] * weights, 0.0
                )

        gradient = jnp.zeros((2 * NAO, NAV), jnp.float32)
        for s in range(n):
            chosen = [tab[s, l:l + 1, :] == lanes_i for l in range(MAXEXC)]
            spread = []
            for j in range(MAXEXC):
                total = jnp.zeros((NAO, dets), jnp.float32)
                for l in range(MAXEXC):
                    total = jnp.where(
                        chosen[l], mats[j * MAXEXC + l, s:s + 1, :], total
                    )
                upper = total.astype(jnp.bfloat16)
                lower = (total - upper.astype(jnp.float32)).astype(jnp.bfloat16)
                spread.append(jnp.concatenate([upper, lower], axis=0))
            gradient = gradient + lax.dot_general(
                jnp.concatenate(spread, axis=1),
                particle_hot(s),
                (((1,), (1,)), ((), ())),
                preferred_element_type=jnp.float32,
            )
        gradient = gradient[:NAO] + gradient[NAO:]
        packed = jnp.concatenate([gradient[:NAO // 2], gradient[NAO // 2:]], axis=1)
        gsend[...] = packed.astype(jnp.bfloat16)
        grecv[me] = packed.astype(jnp.bfloat16)

        grad_copies = []
        for k in range(1, n):
            copy = pltpu.make_async_remote_copy(
                src_ref=gsend,
                dst_ref=grecv.at[me],
                send_sem=grad_s.at[k],
                recv_sem=grad_r.at[k],
                device_id={"det": lax.rem(me + k, n)},
                device_id_type=MESH,
            )
            copy.start()
            grad_copies.append(copy)

        state["corr"], state["grads"] = corr, grad_copies
        acc[...] = jnp.zeros_like(acc)
        acc2[...] = jnp.zeros_like(acc2)
        gpad[...] = jnp.zeros_like(gpad)

    def active_dots():
        for copy in state["grads"]:
            copy.wait_recv()
        low = offset - first
        for s in range(n):
            value = grecv[s].astype(jnp.float32)
            gpad[s, low:low + NAO // 2, 0:NAV] = value[:, 0:NAV]
            gpad[s, low + NAO // 2:low + NAO, 0:NAV] = value[:, NAV:]
        for start in range(first, nocc, BLOCK):
            right = gpad[:, start - first:start - first + BLOCK, :].astype(jnp.bfloat16)
            add_block(acc2, start, right.reshape(n * BLOCK, 128)[:, 0:NAV], NAV)

        state["active"] = diagonal(acc2)

    def whole_dots(c):
        starts = list(range(c * rows, min((c + 1) * rows, nocc), BLOCK))
        full = [start for start in starts if start + BLOCK <= nocc]
        for part in range(4):
            size = vectors * BLOCK // 4
            total = 0.0
            for start in full:
                right = gbuf[:, start:start + BLOCK, 0:nvir].reshape(n * BLOCK, nvir)
                low_i = start + part * (BLOCK // 4)
                left = chol[low_i:low_i + BLOCK // 4].reshape(size, nvir)
                total = total + lax.dot_general(
                    left, right, (((1,), (1,)), ((), ())),
                    preferred_element_type=jnp.float32,
                )
            acc[part * size:(part + 1) * size, :] += total
        for start in starts[len(full):]:
            right = gbuf[:, start:start + BLOCK, 0:nvir].reshape(n * BLOCK, nvir)
            add_block(acc, start, right, nvir)

    events = [(MINORS_AT, pick_minors), (GRADIENT_AT, differentiate)]
    for copy in chol_copies:
        events.append((GRADIENT_AT, copy.wait))
    for c in range(chunks):
        lag = SKEW * c
        events.append((lag, functools.partial(begin, c)))
        for hop in range(1, half + 1):
            events.append((hop + lag, functools.partial(relay, hop, c)))
        events.append((half + lag + 0.01, functools.partial(whole_dots, c)))
    events.append((half + ACTIVE_AFTER, active_dots))
    for _, event in sorted(events, key=lambda item: item[0]):
        event()
    corr, grad_copies = state["corr"], state["grads"]
    whole_part = diagonal(acc)
    both = jnp.concatenate([whole_part, state["active"]], axis=1)
    for w in range(n):
        rsend[w] = both[w:w + 1, :]
    rrecv[me] = rsend[me]
    res_copies = all_to_peers(rsend, rrecv, res_s, res_r, lambda peer: peer)
    corr_out[0] = corr[0, 0]
    for copy in res_copies:
        copy.wait_recv()
    for s in range(n):
        value = rrecv[s]
        bias_out[0:1, s * vectors:(s + 1) * vectors] = (
            corr * value[:, 0:vectors] + value[:, vectors:]
        )
    for copies in (tab_copies, grad_copies, res_copies, ring_copies.values()):
        for copy in copies:
            copy.wait_send()


def solution(mesh):
    n = mesh.shape["det"]

    def shards(greens, chol_vectors, holes, particles, order, amplitudes):
        vectors, nvir, nocc = chol_vectors.shape
        dets = holes.shape[0]
        rows = CHUNK_BLOCKS * BLOCK
        chunks = -(-nocc // rows)
        lanes = -(-nvir // 128) * 128
        first = (nocc - NAO) // BLOCK * BLOCK
        pad_rows = -(-(nocc - first) // BLOCK) * BLOCK
        half = max(1, n // 2)
        vmem = pl.BlockSpec(memory_space=pltpu.VMEM)
        dma = pltpu.SemaphoreType.DMA
        return pl.pallas_call(
            functools.partial(kernel, n, chunks),
            out_shape=(
                jax.ShapeDtypeStruct((1,), jnp.float32),
                jax.ShapeDtypeStruct((1, n * vectors), jnp.float32),
            ),
            in_specs=[vmem, pl.BlockSpec(memory_space=pl.ANY)] + [vmem] * 4,
            out_specs=(pl.BlockSpec(memory_space=pltpu.SMEM), vmem),
            scratch_shapes=[
                pltpu.VMEM((n, chunks * rows, lanes), jnp.bfloat16),
                pltpu.VMEM((nocc, vectors, nvir), jnp.bfloat16),
                pltpu.VMEM((n, 16, dets), jnp.bfloat16),
                pltpu.VMEM((n, 16, dets), jnp.float32),
                pltpu.VMEM((MAXEXC * MAXEXC, n, dets), jnp.float32),
                pltpu.VMEM((NAO // 2, 2 * NAV), jnp.bfloat16),
                pltpu.VMEM((n, NAO // 2, 2 * NAV), jnp.bfloat16),
                pltpu.VMEM((n, pad_rows, 128), jnp.float32),
                pltpu.VMEM((BLOCK * vectors, n * BLOCK), jnp.float32),
                pltpu.VMEM((BLOCK * vectors, n * BLOCK), jnp.float32),
                pltpu.VMEM((n, 1, 2 * vectors), jnp.float32),
                pltpu.VMEM((n, 1, 2 * vectors), jnp.float32),
                dma((chunks,)),
                dma((n,)),
                dma((n,)),
                dma((2, half, chunks)),
                dma((2, half, chunks)),
                dma((n,)),
                dma((n,)),
                dma((n,)),
                dma((n,)),
            ],
            compiler_params=pltpu.CompilerParams(
                collective_id=0, has_side_effects=True
            ),
        )(
            jnp.transpose(greens, (0, 2, 1)),
            jnp.transpose(chol_vectors, (2, 0, 1)),
            holes.T,
            particles.T,
            order.reshape(1, dets),
            amplitudes.reshape(1, dets),
        )

    placed = (
        P(("grp", "det", "wlk"), None, None),
        P(("grp", "det"), None, None),
        P(("grp", "det"), None),
        P(("grp", "det"), None),
        P(("grp", "det")),
        P(("grp", "det")),
    )
    return jax.shard_map(
        shards,
        mesh=mesh,
        in_specs=placed,
        out_specs=(P(("grp", "det", "wlk")), P(("grp", "det", "wlk"), None)),
        check_vma=False,
    )
```
